32 devices in a mesh: dp: 2 (over x), tp: 16 (over z, y, core).
Axes of the slice: x: 2, y: 2, z: 4, core: 2. Of those that a mesh axis runs over, the one named last changes fastest.
Arguments:
- x_in: bfloat16 [8, 1024, 2560], P('dp', 'tp'), parts along dimension 0
- rope_angle: float32 [1024, 32], replicated
- ln_gain: float32 [2560], replicated
- ln_bias: float32 [2560], replicated
- w_q: bfloat16 [2560, 2560], P(None, 'tp')
- b_q: float32 [32, 80], P('tp')
- w_k: bfloat16 [2560, 2560], P(None, 'tp')
- b_k: float32 [32, 80], P('tp')
- w_v: bfloat16 [2560, 2560], P(None, 'tp')
- b_v: float32 [32, 80], P('tp')
- w_o: bfloat16 [2560, 2560], P('tp')
- b_o: float32 [2560], replicated
- w_up: bfloat16 [2560, 10240], P(None, 'tp')
- b_up: float32 [10240], P('tp')
- w_down: bfloat16 [10240, 2560], P('tp')
- b_down: float32 [2560], replicated
- dy_out: bfloat16 [8, 1024, 2560], P('dp', 'tp'), parts along dimension 0
Outputs:
- output 1: bfloat16 [8, 1024, 2560], P('dp', 'tp'), parts along dimension 0
- output 2: float32 [8, 1024, 2560], P('dp', 'tp'), parts along dimension 0
- output 3: float32 [5120], P('dp'), parts along dimension 0
- output 4: float32 [5120], P('dp'), parts along dimension 0
- output 5: float32 [5120, 2560], P('dp', 'tp'), parts along dimension 0
- output 6: float32 [64, 80], P(('dp', 'tp')), parts along dimension 0
- output 7: float32 [5120, 2560], P('dp', 'tp'), parts along dimension 0
- output 8: float32 [64, 80], P(('dp', 'tp')), parts along dimension 0
- output 9: float32 [5120, 2560], P('dp', 'tp'), parts along dimension 0
- output 10: float32 [64, 80], P(('dp', 'tp')), parts along dimension 0
- output 11: float32 [5120, 2560], P(('dp', 'tp')), parts along dimension 0
- output 12: float32 [5120], P('dp'), parts along dimension 0
- output 13: float32 [5120, 10240], P('dp', 'tp'), parts along dimension 0
- output 14: float32 [20480], P(('dp', 'tp')), parts along dimension 0
- output 15: float32 [20480, 2560], P(('dp', 'tp')), parts along dimension 0
- output 16: float32 [5120], P('dp'), parts along dimension 0
There are 2 independent parts. The reference program is written for one: setup_inputs(seed, part) draws one part's arguments, and reference() takes and returns one part's arrays. A program takes and returns all parts, laid end to end along the dimension named above; an argument that names none is the same for every part.
All inputs are finite; a program needn't handle non-finite values.
Results may differ from the reference program's by a relative error of at most 0.02.
Values are sent between devices in bfloat16 or wider.
A program may use at most 1 GiB of HBM per device.

```python
import jax
import jax.numpy as jnp
from jax import lax

NUM_SEQS = 4
SEQ_LEN = 1024
MODEL_DIM = 2560
NUM_HEADS = 32
ROT_DIM = 64
FFN_DIM = 10240

HEAD_DIM = MODEL_DIM // NUM_HEADS
HALF_ROT = ROT_DIM // 2
LN_EPS = 1e-5
ROPE_BASE = 10000.0


def setup_inputs(seed: int = 0, part: int = 0) -> dict:
    base_key = jax.random.key(seed)
    shared_keys = jax.random.split(base_key, 15)
    part_keys = jax.random.split(jax.random.fold_in(base_key, part), 3)

    def normal(rng_key, arr_shape):
        return jax.random.normal(rng_key, arr_shape, jnp.float32)

    def weight(rng_key, fan_in, fan_out):
        return (normal(rng_key, (fan_in, fan_out)) * fan_in ** -0.5).astype(jnp.bfloat16)

    pos_gaps = jax.random.randint(shared_keys[0], (SEQ_LEN,), 1, 5)
    positions = jnp.cumsum(pos_gaps).astype(jnp.float32)
    inv_freq = ROPE_BASE ** (-jnp.arange(0, ROT_DIM, 2).astype(jnp.float32) / ROT_DIM)
    tok_scale = jnp.exp(0.5 * normal(part_keys[0], (NUM_SEQS, SEQ_LEN, 1)))
    act_shape = (NUM_SEQS, SEQ_LEN, MODEL_DIM)
    head_shape = (NUM_HEADS, HEAD_DIM)
    return {
        'x_in': (normal(part_keys[1], act_shape) * tok_scale).astype(jnp.bfloat16),
        'rope_angle': positions[:, None] * inv_freq[None, :],
        'ln_gain': 1.0 + 0.2 * normal(shared_keys[1], (MODEL_DIM,)),
        'ln_bias': 0.5 * normal(shared_keys[2], (MODEL_DIM,)),
        'w_q': weight(shared_keys[3], MODEL_DIM, MODEL_DIM),
        'b_q': 0.5 * normal(shared_keys[4], head_shape),
        'w_k': weight(shared_keys[5], MODEL_DIM, MODEL_DIM),
        'b_k': 0.5 * normal(shared_keys[6], head_shape),
        'w_v': weight(shared_keys[7], MODEL_DIM, MODEL_DIM),
        'b_v': 0.5 * normal(shared_keys[8], head_shape),
        'w_o': weight(shared_keys[9], MODEL_DIM, MODEL_DIM),
        'b_o': 0.5 * normal(shared_keys[10], (MODEL_DIM,)),
        'w_up': weight(shared_keys[11], MODEL_DIM, FFN_DIM),
        'b_up': 0.5 * normal(shared_keys[12], (FFN_DIM,)),
        'w_down': weight(shared_keys[13], FFN_DIM, MODEL_DIM),
        'b_down': 0.5 * normal(shared_keys[14], (MODEL_DIM,)),
        'dy_out': normal(part_keys[2], act_shape).astype(jnp.bfloat16),
    }


def to_bf16(t):
    return t.astype(jnp.bfloat16).astype(jnp.float32)


def rope_rotate(t, cos_t, sin_t):
    t_rot = t[..., :ROT_DIM]
    turned = jnp.concatenate([-t_rot[..., HALF_ROT:], t_rot[..., :HALF_ROT]], axis=-1)
    return jnp.concatenate([t_rot * cos_t + turned * sin_t, t[..., ROT_DIM:]], axis=-1)


def head_attention(triple):
    q_head, k_head, v_head = triple
    seq_pos = jnp.arange(SEQ_LEN)
    scores = jnp.einsum('bqd,bkd->bqk', q_head, k_head) * HEAD_DIM ** -0.5
    scores = jnp.where(seq_pos[:, None] >= seq_pos[None, :], scores, -1e30)
    prob_mat = to_bf16(jax.nn.softmax(scores, axis=-1))
    return to_bf16(jnp.einsum('bqk,bkd->bqd', prob_mat, v_head))


def layer_forward(x_f, ln_gain, ln_bias, w_q, b_q, w_k, b_k, w_v, b_v, w_o, b_o, w_up, b_up, w_down, b_down, cos_t, sin_t):
    centered = x_f - jnp.mean(x_f, axis=-1, keepdims=True)
    inv_std = lax.rsqrt(jnp.mean(centered * centered, axis=-1, keepdims=True) + LN_EPS)
    h_flat = to_bf16(centered * inv_std * ln_gain + ln_bias).reshape(NUM_SEQS * SEQ_LEN, MODEL_DIM)

    def project(w_mat, b_vec):
        linear = jnp.dot(h_flat, w_mat, preferred_element_type=jnp.float32)
        return to_bf16(linear.reshape(NUM_SEQS, SEQ_LEN, NUM_HEADS, HEAD_DIM) + b_vec)

    q_r = to_bf16(rope_rotate(project(w_q, b_q), cos_t, sin_t))
    k_r = to_bf16(rope_rotate(project(w_k, b_k), cos_t, sin_t))
    v_p = project(w_v, b_v)
    heads_first = (jnp.transpose(q_r, (2, 0, 1, 3)), jnp.transpose(k_r, (2, 0, 1, 3)), jnp.transpose(v_p, (2, 0, 1, 3)))
    context = lax.map(jax.checkpoint(head_attention), heads_first)
    ctx_flat = jnp.transpose(context, (1, 2, 0, 3)).reshape(NUM_SEQS * SEQ_LEN, MODEL_DIM)
    act_bf = to_bf16(jax.nn.gelu(jnp.dot(h_flat, w_up, preferred_element_type=jnp.float32) + b_up, approximate=True))
    y_flat = (x_f.reshape(NUM_SEQS * SEQ_LEN, MODEL_DIM)
              + jnp.dot(ctx_flat, w_o, preferred_element_type=jnp.float32)
              + jnp.dot(act_bf, w_down, preferred_element_type=jnp.float32)
              + b_o + b_down)
    return y_flat.reshape(NUM_SEQS, SEQ_LEN, MODEL_DIM)


def reference(x_in, rope_angle, ln_gain, ln_bias, w_q, b_q, w_k, b_k, w_v, b_v, w_o, b_o, w_up, b_up, w_down, b_down, dy_out):
    angle_pair = jnp.concatenate([rope_angle, rope_angle], axis=-1)[None, :, None, :]
    cos_t = jnp.cos(angle_pair)
    sin_t = jnp.sin(angle_pair)
    primals = (x_in.astype(jnp.float32), ln_gain, ln_bias,
               w_q.astype(jnp.float32), b_q, w_k.astype(jnp.float32), b_k,
               w_v.astype(jnp.float32), b_v, w_o.astype(jnp.float32), b_o,
               w_up.astype(jnp.float32), b_up, w_down.astype(jnp.float32), b_down)
    y_f, pull_back = jax.vjp(lambda *values_in: layer_forward(*values_in, cos_t, sin_t), *primals)
    all_grads = pull_back(dy_out.astype(jnp.float32))
    return (y_f.astype(jnp.bfloat16), all_grads[0], all_grads[1], all_grads[2], all_grads[3],
            all_grads[4], all_grads[5], all_grads[6], all_grads[7], all_grads[8], all_grads[9],
            all_grads[10], all_grads[11], all_grads[12], all_grads[13], all_grads[14])
```

```python
import jax
import jax.numpy as jnp
from jax import lax
from jax.experimental import pallas as pl
from jax.experimental.layout import Layout, with_layout_constraint
from jax.experimental.pallas import tpu as pltpu
from jax.sharding import PartitionSpec as P

LN_EPS = 1e-5
HEAD = 80
HALF = 32
LANES = 128
Q_BLK = 256
RING = (0, 2, 4, 6, 7, 5, 3, 1)
N_CHIP = 8
VMEM_LIMIT = 60 * 2 ** 20


def norm_stats(x_blk):
    x_f = x_blk.astype(jnp.float32)
    centered = x_f - jnp.mean(x_f, axis=-1, keepdims=True)
    inv_std = lax.rsqrt(jnp.mean(centered * centered, axis=-1, keepdims=True) + LN_EPS)
    return centered * inv_std, inv_std


def norm_backward(d_h, normed, inv_std, ln_gain):
    d_norm = d_h * ln_gain
    return inv_std * (d_norm - jnp.mean(d_norm, axis=-1, keepdims=True)
                      - normed * jnp.mean(d_norm * normed, axis=-1, keepdims=True))


def gelu_tanh(t):
    return jax.nn.gelu(t, approximate=True)


def lane_iota(rows):
    return lax.broadcasted_iota(jnp.int32, (rows, LANES), 1)


def unpack_head(ref, offset):
    rows = ref.shape[0]
    col, shift = offset // LANES, offset % LANES
    lane = lane_iota(rows)
    head = ref[:, col * LANES:(col + 1) * LANES].astype(jnp.float32)
    if shift:
        head = pltpu.roll(head, LANES - shift, 1)
        if shift + HEAD > LANES:
            after = pltpu.roll(ref[:, (col + 1) * LANES:(col + 2) * LANES].astype(jnp.float32), LANES - shift, 1)
            head = jnp.where(lane < LANES - shift, head, after)
    return jnp.where(lane < HEAD, head, 0.0)


def pack_heads(heads, n_cols):
    rows = heads[0].shape[0]
    lane = lane_iota(rows)
    cols = [None] * n_cols
    for idx, head in enumerate(heads):
        offset = idx * HEAD
        col, shift = offset // LANES, offset % LANES
        moved = pltpu.roll(head, shift, 1) if shift else head
        low = (lane >= shift) & (lane < shift + HEAD)
        cols[col] = jnp.where(low, moved, 0.0 if cols[col] is None else cols[col])
        if shift + HEAD > LANES:
            cols[col + 1] = jnp.where(lane < shift + HEAD - LANES, moved, 0.0)
    return cols


def rotate(t, cos_t, sin_up, sin_down):
    return t * cos_t + pltpu.roll(t, HALF, 1) * sin_up + pltpu.roll(t, LANES - HALF, 1) * sin_down


def dot_nt(a, b):
    return lax.dot_general(a, b, (((1,), (1,)), ((), ())), preferred_element_type=jnp.float32)


def dot_nn(a, b):
    return jnp.dot(a, b, preferred_element_type=jnp.float32)


def causal(hi, lo):
    key = lax.broadcasted_iota(jnp.int32, (hi, Q_BLK), 0)
    query = lax.broadcasted_iota(jnp.int32, (hi, Q_BLK), 1) + lo
    return key <= query


def attn_fwd_kernel(qkv_ref, cos_ref, up_ref, down_ref, ctx_ref, lse_ref, head_scr):
    seq = qkv_ref.shape[0]
    scale = HEAD ** -0.5
    cos_t, sin_up, sin_down = cos_ref[...], up_ref[...], down_ref[...]
    lse_ref[...] = jnp.zeros_like(lse_ref)
    for h in range(2):
        q = rotate(unpack_head(qkv_ref, h * HEAD), cos_t, sin_up, sin_down).astype(jnp.bfloat16)
        k = rotate(unpack_head(qkv_ref, (2 + h) * HEAD), cos_t, sin_up, sin_down).astype(jnp.bfloat16)
        v_t = unpack_head(qkv_ref, (4 + h) * HEAD).T.astype(jnp.bfloat16)
        for lo in range(0, seq, Q_BLK):
            hi = lo + Q_BLK
            s_t = dot_nt(k[:hi], q[lo:hi]) * scale
            s_t = jnp.where(causal(hi, lo), s_t, -1e30)
            top = jnp.max(s_t, axis=0, keepdims=True)
            e_t = jnp.exp(s_t - top)
            total = jnp.sum(e_t, axis=0, keepdims=True)
            p_t = (e_t * (1.0 / total)).astype(jnp.bfloat16)
            head_scr[h, lo:hi, :] = dot_nn(v_t[:, :hi], p_t).T
            lse_ref[h:h + 1, lo:hi] = top + jnp.log(total)
    cols = pack_heads([head_scr[0], head_scr[1]], 2)
    for c in range(2):
        ctx_ref[:, c * LANES:(c + 1) * LANES] = cols[c].astype(jnp.bfloat16)


def attn_bwd_kernel(qkv_ref, dctx_ref, lse_ref, cos_ref, up_ref, down_ref, dqkv_ref, dbias_ref, d_scr):
    seq = qkv_ref.shape[0]
    scale = HEAD ** -0.5
    cos_t, sin_up, sin_down = cos_ref[...], up_ref[...], down_ref[...]
    for h in range(2):
        q = rotate(unpack_head(qkv_ref, h * HEAD), cos_t, sin_up, sin_down).astype(jnp.bfloat16)
        k_f = rotate(unpack_head(qkv_ref, (2 + h) * HEAD), cos_t, sin_up, sin_down)
        k = k_f.astype(jnp.bfloat16)
        k_t = k_f.T.astype(jnp.bfloat16)
        v = unpack_head(qkv_ref, (4 + h) * HEAD).astype(jnp.bfloat16)
        dctx = unpack_head(dctx_ref, h * HEAD).astype(jnp.bfloat16)
        for lo in reversed(range(0, seq, Q_BLK)):
            hi = lo + Q_BLK
            s_t = dot_nt(k[:hi], q[lo:hi]) * scale
            p_t = jnp.where(causal(hi, lo), jnp.exp(s_t - lse_ref[h:h + 1, lo:hi]), 0.0)
            dp_t = dot_nt(v[:hi], dctx[lo:hi])
            row = jnp.sum(dp_t * p_t, axis=0, keepdims=True)
            ds_t = (p_t * (dp_t - row) * scale).astype(jnp.bfloat16)
            d_scr[h, lo:hi, :] = dot_nn(k_t[:, :hi], ds_t).T
            dk_part = dot_nn(ds_t, q[lo:hi])
            dv_part = dot_nn(p_t.astype(jnp.bfloat16), dctx[lo:hi])
            if hi == seq:
                d_scr[2 + h] = dk_part
                d_scr[4 + h] = dv_part
            else:
                d_scr[2 + h, :hi, :] += dk_part
                d_scr[4 + h, :hi, :] += dv_part
    heads = [rotate(d_scr[j], cos_t, -sin_up, -sin_down) for j in range(4)] + [d_scr[4], d_scr[5]]
    cols = pack_heads(heads, 4)
    for c in range(4):
        span = slice(c * LANES, (c + 1) * LANES)
        dqkv_ref[:, span] = cols[c].astype(jnp.bfloat16)
        dbias_ref[:, span] = jnp.broadcast_to(jnp.sum(cols[c], axis=0, keepdims=True), (8, LANES))


def seq_spec(rows, width):
    return pl.BlockSpec((None, rows, width), lambda b: (b, 0, 0))


def table_spec(rows):
    return pl.BlockSpec((rows, LANES), lambda b: (0, 0))


def attn_fwd(qkv, tables):
    n_seq, seq, _ = qkv.shape
    return pl.pallas_call(
        attn_fwd_kernel,
        grid=(n_seq,),
        in_specs=[seq_spec(seq, 512)] + [table_spec(seq)] * 3,
        out_specs=[seq_spec(seq, 256), seq_spec(8, seq)],
        out_shape=[jax.ShapeDtypeStruct((n_seq, seq, 256), jnp.bfloat16),
                   jax.ShapeDtypeStruct((n_seq, 8, seq), jnp.float32)],
        scratch_shapes=[pltpu.VMEM((2, seq, LANES), jnp.float32)],
        compiler_params=pltpu.CompilerParams(vmem_limit_bytes=VMEM_LIMIT),
        cost_estimate=pl.CostEstimate(flops=15 * 10 ** 9, bytes_accessed=8 * 10 ** 6, transcendentals=6 * 10 ** 6),
        name="attn_fwd",
    )(qkv, *tables)


def attn_bwd(qkv, dctx, lse, tables, first, count, done=None):
    n_seq, seq, _ = qkv.shape

    def rows(n, width):
        return pl.BlockSpec((None, n, width), lambda b: (b + first, 0, 0))

    ins = [qkv, dctx, lse, *tables]
    in_specs = [rows(seq, 512), rows(seq, 256), rows(8, seq)] + [table_spec(seq)] * 3
    kernel, aliases = attn_bwd_kernel, {}
    if done is not None:
        aliases = {len(ins): 0, len(ins) + 1: 1}
        ins += done
        in_specs += [pl.BlockSpec(memory_space=pl.ANY)] * 2

        def kernel(*refs):
            attn_bwd_kernel(*refs[:6], *refs[8:])

    return pl.pallas_call(
        kernel,
        grid=(count,),
        in_specs=in_specs,
        out_specs=[rows(seq, 512), rows(8, 512)],
        out_shape=[jax.ShapeDtypeStruct((n_seq, seq, 512), jnp.bfloat16),
                   jax.ShapeDtypeStruct((n_seq, 8, 512), jnp.float32)],
        scratch_shapes=[pltpu.VMEM((6, seq, LANES), jnp.float32)],
        input_output_aliases=aliases,
        compiler_params=pltpu.CompilerParams(vmem_limit_bytes=VMEM_LIMIT),
        cost_estimate=pl.CostEstimate(flops=15 * 10 ** 9, bytes_accessed=12 * 10 ** 6, transcendentals=6 * 10 ** 6),
        name="attn_bwd",
    )(*ins)


def rope_tables(rope_angle):
    cos_a, sin_a = jnp.cos(rope_angle), jnp.sin(rope_angle)
    rows = rope_angle.shape[0]
    zero = jnp.zeros((rows, HALF), jnp.float32)
    ones = jnp.ones((rows, LANES - 2 * HALF), jnp.float32)
    return (jnp.concatenate([cos_a, cos_a, ones], axis=1),
            jnp.concatenate([zero, sin_a, 0.0 * ones], axis=1),
            jnp.concatenate([-sin_a, zero, 0.0 * ones], axis=1))


def ring_perm(step):
    return [(RING[r] * 2 + c, RING[(r + step) % N_CHIP] * 2 + c) for r in range(N_CHIP) for c in range(2)]


PARTNER = [(t, t ^ 1) for t in range(2 * N_CHIP)]


def ring_place():
    tp = lax.axis_index('tp')
    chip, core = tp // 2, tp % 2
    return jnp.where(chip % 2 == 0, chip // 2, 7 - chip // 2), core


def chip_at(place):
    place = place % N_CHIP
    return jnp.where(place < 4, place * 2, 15 - place * 2)


def tie(values, after):
    return lax.optimization_barrier((*values, after))[:-1]


def product_kernel(n_parts, n_blk, idx_ref, *refs):
    del idx_ref
    w_ref, theirs_ref, own_ref, rows_scr = refs[n_blk * n_parts], *refs[n_blk * n_parts + 1:]

    @pl.when(pl.program_id(0) == 0)
    def _():
        base = 0
        for p in range(n_parts):
            depth = refs[n_blk * p].shape[-1]
            for j in range(n_blk):
                blk = refs[n_blk * p + j].shape[0]
                rows_scr[j * blk:(j + 1) * blk, base:base + depth] = refs[n_blk * p + j][...]
            base += depth

    half = rows_scr.shape[0] // 2
    theirs_ref[...] = dot_nn(rows_scr[:half, :], w_ref[...]).astype(jnp.bfloat16).reshape(theirs_ref.shape)
    own_ref[...] = dot_nn(rows_scr[half:, :], w_ref[...]).astype(jnp.bfloat16).reshape(own_ref.shape)


def block_products(parts, w_mat, idx):
    n_seq, seq_len, _ = parts[0].shape
    depth, n_out = w_mat.shape
    blk, tile, hops = seq_len // (2 * N_CHIP), 512, 2
    in_specs, ins = [], []
    for part in parts:
        for which in range(2):
            for hop in range(hops):
                for seq in range(n_seq):
                    pos = (which * hops + hop) * 2 + seq // (n_seq // 2)
                    in_specs.append(pl.BlockSpec((None, blk, part.shape[-1]),
                                                 lambda n, idx, seq=seq, pos=pos: (seq, idx[pos], 0)))
                    ins.append(part)
    in_specs.append(pl.BlockSpec((depth, tile), lambda n, idx: (0, n)))
    out_spec = pl.BlockSpec((hops, n_seq, blk, tile), lambda n, idx: (0, 0, 0, n))
    shape = jax.ShapeDtypeStruct((hops, n_seq, blk, n_out), jnp.bfloat16)
    n_parts, n_blk = len(parts), 2 * hops * n_seq

    def kernel(*refs):
        product_kernel(n_parts, n_blk, *refs)

    return pl.pallas_call(
        kernel,
        grid_spec=pltpu.PrefetchScalarGridSpec(
            num_scalar_prefetch=1, grid=(n_out // tile,), in_specs=in_specs, out_specs=[out_spec, out_spec],
            scratch_shapes=[pltpu.VMEM((n_blk * blk, depth), jnp.bfloat16)]),
        out_shape=[shape, shape],
        compiler_params=pltpu.CompilerParams(vmem_limit_bytes=VMEM_LIMIT),
        cost_estimate=pl.CostEstimate(flops=2 * n_blk * blk * depth * n_out, bytes_accessed=2 * depth * n_out, transcendentals=0),
        name="block_products",
    )(idx, *ins, w_mat)


def hop_sums_kernel(n_got, *refs):
    for j in range(2):
        total = refs[2 * j][...].astype(jnp.float32) + refs[2 * j + 1][...].astype(jnp.float32)
        if n_got:
            total = total + refs[4 + j][...].astype(jnp.float32)
        refs[4 + n_got + j][...] = total.astype(refs[4 + n_got + j].dtype)


def hop_sums(own, theirs, hop, got, dtype):
    _, n_seq, blk, n_out = own.shape
    half = n_seq // 2
    in_specs, ins = [], []
    for j in range(2):
        for t in (own, theirs):
            in_specs.append(pl.BlockSpec((None, None, blk, n_out), lambda i, j=j: (hop, j * half + i, 0, 0)))
            ins.append(t)
    one = pl.BlockSpec((None, blk, n_out), lambda i: (i, 0, 0))
    shape = jax.ShapeDtypeStruct((half, blk, n_out), dtype)
    n_got = len(got)

    def kernel(*refs):
        hop_sums_kernel(n_got, *refs)

    return pl.pallas_call(
        kernel,
        grid=(half,),
        in_specs=in_specs + [one] * n_got,
        out_specs=[one, one],
        out_shape=[shape, shape],
        compiler_params=pltpu.CompilerParams(vmem_limit_bytes=16 * 2 ** 20),
        cost_estimate=pl.CostEstimate(flops=10 ** 7, bytes_accessed=6 * 10 ** 6, transcendentals=0),
        name="hop_sums",
    )(*ins, *got)


def matmul_scatter(parts, w_mat, fillers, ahead, results, first_after=None):
    half = parts[0].shape[0] // 2
    place, core = ring_place()
    products = {}

    def start_product(step, token):
        chips = [chip_at(place + side * (1 + s)) * 2 for s in (step, step + 1) for side in (-1, 1)]
        idx = jnp.stack([c + 1 - core for c in chips] + [c + core for c in chips]).astype(jnp.int32)
        if token is not None:
            idx, = tie((idx,), token)
        theirs, own = block_products(parts, w_mat, idx)
        products[step] = own, lax.ppermute(theirs, 'tp', PARTNER)

    for step in range(0, min(ahead, N_CHIP), 2):
        start_product(step, None)
    got = ()
    for step in range(N_CHIP):
        own, theirs = products[step - step % 2]
        last = step == N_CHIP - 1
        send_a, send_b = hop_sums(own, theirs, step % 2, got, jnp.float32 if last else jnp.bfloat16)
        if not last:
            if step == 0 and first_after is not None:
                send_a, send_b = tie((send_a, send_b), first_after)
            got_a = lax.ppermute(send_a, 'tp', ring_perm(1))
            got_b = lax.ppermute(send_b, 'tp', ring_perm(-1))
            if step % 2 == 0 and step + ahead < N_CHIP:
                start_product(step + ahead, send_a)
            if step < len(fillers) and fillers[step] is not None:
                made = fillers[step](send_a)
                got_a, *values = lax.optimization_barrier((got_a, *made.values()))
                results.update(zip(made, values))
            got = (got_a, got_b)
    return jnp.concatenate([send_a, send_b], axis=0)


def small_all_reduce(t):
    for bit in (1, 2, 4, 8):
        t = t + lax.ppermute(t, 'tp', [(d, d ^ bit) for d in range(2 * N_CHIP)])
    return t


def rows_major(t):
    return with_layout_constraint(t, Layout(major_to_minor=tuple(range(t.ndim))))


def layer_body(x_blk, rope_angle, ln_gain, ln_bias, w_q, b_q, w_k, b_k, w_v, b_v, w_o, b_o, w_up, b_up, w_down, b_down, dy_blk):
    normed, inv_std = norm_stats(x_blk)
    h_loc = (normed * ln_gain + ln_bias).astype(jnp.bfloat16)
    h_full = lax.all_gather(h_loc, 'tp', axis=1, tiled=True)
    dy_full = lax.all_gather(dy_blk, 'tp', axis=1, tiled=True)
    n_seq, seq_len, model_dim = h_full.shape
    heads_loc, head_dim = b_q.shape
    width = heads_loc * head_dim
    tables = rope_tables(rope_angle)

    w_qkv = jnp.concatenate([w_q, w_k, w_v, jnp.zeros((model_dim, 32), jnp.bfloat16)], axis=1)
    b_qkv = jnp.concatenate([b_q.reshape(-1), b_k.reshape(-1), b_v.reshape(-1), jnp.zeros((32,), jnp.float32)])
    w_o_pad = jnp.concatenate([w_o, jnp.zeros((256 - width, model_dim), jnp.bfloat16)], axis=0)
    w_out = rows_major(jnp.concatenate([w_o_pad, w_down], axis=0))
    w_in_t = rows_major(jnp.concatenate([w_qkv, w_up], axis=1).T)

    qkv = (jnp.einsum('bsd,de->bse', h_full, w_qkv, preferred_element_type=jnp.float32) + b_qkv).astype(jnp.bfloat16)
    ctx, lse = attn_fwd(qkv, tables)
    act_f, gelu_pull = jax.vjp(gelu_tanh, jnp.einsum('bsd,df->bsf', h_full, w_up, preferred_element_type=jnp.float32) + b_up)
    act_bf = act_f.astype(jnp.bfloat16)
    act_bf = rows_major(act_bf)
    out = {}

    def run_dctx(token):
        dy_t, = tie((dy_full,), token)
        return {'d_ctx': jnp.einsum('bse,ce->bsc', dy_t, w_o_pad, preferred_element_type=jnp.float32).astype(jnp.bfloat16)}

    def run_attn_a(token):
        d_ctx, = tie((out['d_ctx'],), token)
        return dict(zip(('d_qkv', 'd_bias'), attn_bwd(qkv, d_ctx, lse, tables, 0, 2)))

    def run_attn_b(token):
        d_ctx, = tie((out['d_ctx'],), token)
        return dict(zip(('d_qkv', 'd_bias'), attn_bwd(qkv, d_ctx, lse, tables, 2, 2, [out['d_qkv'], out['d_bias']])))

    def run_dact(token):
        dy_t, = tie((dy_full,), token)
        d_pre = gelu_pull(jnp.einsum('bse,fe->bsf', dy_t, w_down, preferred_element_type=jnp.float32))[0]
        return {'grad_bup': jnp.sum(d_pre, axis=(0, 1)), 'd_pre': rows_major(d_pre.astype(jnp.bfloat16))}

    branch_sum = matmul_scatter((ctx, act_bf), w_out, (run_dctx, run_attn_a, run_attn_b, run_dact), N_CHIP, out, dy_full)
    y_blk = (x_blk.astype(jnp.float32) + branch_sum + b_o + b_down).astype(jnp.bfloat16)

    d_qkv, d_bias, d_pre_bf = out['d_qkv'], out['d_bias'], out['d_pre']
    dy_f = dy_blk.astype(jnp.float32)

    def run_wdown(token):
        dy_t, = tie((dy_full,), token)
        return {'wdown': jnp.einsum('bsf,bse->fe', act_bf, dy_t, preferred_element_type=jnp.float32)}

    def run_wo(token):
        dy_t, = tie((dy_full,), token)
        return {'wo': jnp.einsum('bsc,bse->ce', ctx, dy_t, preferred_element_type=jnp.float32)[:width]}

    def run_wup(token):
        h_t, = tie((h_full,), token)
        return {'wup': jnp.einsum('bsd,bsf->df', h_t, d_pre_bf, preferred_element_type=jnp.float32)}

    def run_wqkv(token):
        h_t, = tie((h_full,), token)
        grad = jnp.einsum('bsc,bsd->cd', d_qkv, h_t, preferred_element_type=jnp.float32)
        return {name: grad[j * width:(j + 1) * width] for j, name in enumerate(('wq', 'wk', 'wv'))}

    d_h_loc = matmul_scatter((d_qkv, d_pre_bf), w_in_t, (run_wo, run_wqkv, None, run_wdown, None, run_wup), 2, out)
    grad_wq, grad_wk, grad_wv = out['wq'].T, out['wk'].T, out['wv'].T
    grad_wo, grad_wup, grad_wdown, grad_bup = out['wo'], out['wup'], out['wdown'], out['grad_bup']
    grad_b = jnp.sum(d_bias[:, 0, :], axis=0)
    grad_bq, grad_bk, grad_bv = (grad_b[j * width:(j + 1) * width].reshape(heads_loc, head_dim) for j in range(3))

    small_sums = small_all_reduce(jnp.stack([jnp.sum(d_h_loc * normed, axis=(0, 1)), jnp.sum(d_h_loc, axis=(0, 1)),
                                             jnp.sum(dy_f, axis=(0, 1))]))
    d_x = dy_f + norm_backward(d_h_loc, normed, inv_std, ln_gain)
    return (y_blk, d_x, small_sums[0], small_sums[1], grad_wq, grad_bq, grad_wk, grad_bk,
            grad_wv, grad_bv, grad_wo, small_sums[2], grad_wup, grad_bup, grad_wdown, small_sums[2])


def solution(mesh):
    row_spec = P('dp', 'tp', None)
    col_spec = P(None, 'tp')
    head_spec = P('tp', None)
    grad_cols = P('dp', 'tp')
    grad_rows = P(('dp', 'tp'), None)
    in_specs = (row_spec, P(None, None), P(None), P(None), col_spec, head_spec, col_spec, head_spec,
                col_spec, head_spec, P('tp', None), P(None), col_spec, P('tp'), P('tp', None), P(None), row_spec)
    out_specs = (row_spec, row_spec, P('dp'), P('dp'), grad_cols, grad_rows, grad_cols, grad_rows, grad_cols,
                 grad_rows, grad_rows, P('dp'), grad_cols, P(('dp', 'tp')), grad_rows, P('dp'))
    return jax.shard_map(layer_body, mesh=mesh, in_specs=in_specs, out_specs=out_specs, check_vma=False)
```

```python
import jax
import jax.numpy as jnp
from jax import lax
from jax.experimental import pallas as pl
from jax.experimental.layout import Layout, with_layout_constraint
from jax.experimental.pallas import tpu as pltpu
from jax.sharding import PartitionSpec as P

LN_EPS = 1e-5
HEAD = 80
HALF = 32
LANES = 128
Q_BLK = 256
RING = (0, 2, 4, 6, 7, 5, 3, 1)
N_CHIP = 8
VMEM_LIMIT = 60 * 2 ** 20


def norm_stats(x_blk):
    x_f = x_blk.astype(jnp.float32)
    centered = x_f - jnp.mean(x_f, axis=-1, keepdims=True)
    inv_std = lax.rsqrt(jnp.mean(centered * centered, axis=-1, keepdims=True) + LN_EPS)
    return centered * inv_std, inv_std


def norm_backward(d_h, normed, inv_std, ln_gain):
    d_norm = d_h * ln_gain
    return inv_std * (d_norm - jnp.mean(d_norm, axis=-1, keepdims=True)
                      - normed * jnp.mean(d_norm * normed, axis=-1, keepdims=True))


def gelu_tanh(t):
    return jax.nn.gelu(t, approximate=True)


def lane_iota(rows):
    return lax.broadcasted_iota(jnp.int32, (rows, LANES), 1)


def unpack_head(ref, offset):
    rows = ref.shape[0]
    col, shift = offset // LANES, offset % LANES
    lane = lane_iota(rows)
    head = ref[:, col * LANES:(col + 1) * LANES].astype(jnp.float32)
    if shift:
        head = pltpu.roll(head, LANES - shift, 1)
        if shift + HEAD > LANES:
            after = pltpu.roll(ref[:, (col + 1) * LANES:(col + 2) * LANES].astype(jnp.float32), LANES - shift, 1)
            head = jnp.where(lane < LANES - shift, head, after)
    return jnp.where(lane < HEAD, head, 0.0)


def pack_heads(heads, n_cols):
    rows = heads[0].shape[0]
    lane = lane_iota(rows)
    cols = [None] * n_cols
    for idx, head in enumerate(heads):
        offset = idx * HEAD
        col, shift = offset // LANES, offset % LANES
        moved = pltpu.roll(head, shift, 1) if shift else head
        low = (lane >= shift) & (lane < shift + HEAD)
        cols[col] = jnp.where(low, moved, 0.0 if cols[col] is None else cols[col])
        if shift + HEAD > LANES:
            cols[col + 1] = jnp.where(lane < shift + HEAD - LANES, moved, 0.0)
    return cols


def rotate(t, cos_t, sin_up, sin_down):
    return t * cos_t + pltpu.roll(t, HALF, 1) * sin_up + pltpu.roll(t, LANES - HALF, 1) * sin_down


def dot_nt(a, b):
    return lax.dot_general(a, b, (((1,), (1,)), ((), ())), preferred_element_type=jnp.float32)


def dot_nn(a, b):
    return jnp.dot(a, b, preferred_element_type=jnp.float32)


def causal(hi, lo):
    key = lax.broadcasted_iota(jnp.int32, (hi, Q_BLK), 0)
    query = lax.broadcasted_iota(jnp.int32, (hi, Q_BLK), 1) + lo
    return key <= query


def attn_fwd_kernel(qkv_ref, cos_ref, up_ref, down_ref, ctx_ref, lse_ref, head_scr):
    seq = qkv_ref.shape[0]
    scale = HEAD ** -0.5
    cos_t, sin_up, sin_down = cos_ref[...], up_ref[...], down_ref[...]
    lse_ref[...] = jnp.zeros_like(lse_ref)
    for h in range(2):
        q = rotate(unpack_head(qkv_ref, h * HEAD), cos_t, sin_up, sin_down).astype(jnp.bfloat16)
        k = rotate(unpack_head(qkv_ref, (2 + h) * HEAD), cos_t, sin_up, sin_down).astype(jnp.bfloat16)
        v_t = unpack_head(qkv_ref, (4 + h) * HEAD).T.astype(jnp.bfloat16)
        for lo in range(0, seq, Q_BLK):
            hi = lo + Q_BLK
            s_t = dot_nt(k[:hi], q[lo:hi]) * scale
            s_t = jnp.where(causal(hi, lo), s_t, -1e30)
            top = jnp.max(s_t, axis=0, keepdims=True)
            e_t = jnp.exp(s_t - top)
            total = jnp.sum(e_t, axis=0, keepdims=True)
            p_t = (e_t * (1.0 / total)).astype(jnp.bfloat16)
            head_scr[h, lo:hi, :] = dot_nn(v_t[:, :hi], p_t).T
            lse_ref[h:h + 1, lo:hi] = top + jnp.log(total)
    cols = pack_heads([head_scr[0], head_scr[1]], 2)
    for c in range(2):
        ctx_ref[:, c * LANES:(c + 1) * LANES] = cols[c].astype(jnp.bfloat16)


def attn_bwd_kernel(qkv_ref, dctx_ref, lse_ref, cos_ref, up_ref, down_ref, dqkv_ref, dbias_ref, d_scr):
    seq = qkv_ref.shape[0]
    scale = HEAD ** -0.5
    cos_t, sin_up, sin_down = cos_ref[...], up_ref[...], down_ref[...]
    for h in range(2):
        q = rotate(unpack_head(qkv_ref, h * HEAD), cos_t, sin_up, sin_down).astype(jnp.bfloat16)
        k_f = rotate(unpack_head(qkv_ref, (2 + h) * HEAD), cos_t, sin_up, sin_down)
        k = k_f.astype(jnp.bfloat16)
        k_t = k_f.T.astype(jnp.bfloat16)
        v = unpack_head(qkv_ref, (4 + h) * HEAD).astype(jnp.bfloat16)
        dctx = unpack_head(dctx_ref, h * HEAD).astype(jnp.bfloat16)
        for lo in reversed(range(0, seq, Q_BLK)):
            hi = lo + Q_BLK
            s_t = dot_nt(k[:hi], q[lo:hi]) * scale
            p_t = jnp.where(causal(hi, lo), jnp.exp(s_t - lse_ref[h:h + 1, lo:hi]), 0.0)
            dp_t = dot_nt(v[:hi], dctx[lo:hi])
            row = jnp.sum(dp_t * p_t, axis=0, keepdims=True)
            ds_t = (p_t * (dp_t - row) * scale).astype(jnp.bfloat16)
            d_scr[h, lo:hi, :] = dot_nn(k_t[:, :hi], ds_t).T
            dk_part = dot_nn(ds_t, q[lo:hi])
            dv_part = dot_nn(p_t.astype(jnp.bfloat16), dctx[lo:hi])
            if hi == seq:
                d_scr[2 + h] = dk_part
                d_scr[4 + h] = dv_part
            else:
                d_scr[2 + h, :hi, :] += dk_part
                d_scr[4 + h, :hi, :] += dv_part
    heads = [rotate(d_scr[j], cos_t, -sin_up, -sin_down) for j in range(4)] + [d_scr[4], d_scr[5]]
    cols = pack_heads(heads, 4)
    for c in range(4):
        span = slice(c * LANES, (c + 1) * LANES)
        dqkv_ref[:, span] = cols[c].astype(jnp.bfloat16)
        dbias_ref[:, span] = jnp.broadcast_to(jnp.sum(cols[c], axis=0, keepdims=True), (8, LANES))


def seq_spec(rows, width):
    return pl.BlockSpec((None, rows, width), lambda b: (b, 0, 0))


def table_spec(rows):
    return pl.BlockSpec((rows, LANES), lambda b: (0, 0))


def attn_fwd(qkv, tables):
    n_seq, seq, _ = qkv.shape
    return pl.pallas_call(
        attn_fwd_kernel,
        grid=(n_seq,),
        in_specs=[seq_spec(seq, 512)] + [table_spec(seq)] * 3,
        out_specs=[seq_spec(seq, 256), seq_spec(8, seq)],
        out_shape=[jax.ShapeDtypeStruct((n_seq, seq, 256), jnp.bfloat16),
                   jax.ShapeDtypeStruct((n_seq, 8, seq), jnp.float32)],
        scratch_shapes=[pltpu.VMEM((2, seq, LANES), jnp.float32)],
        compiler_params=pltpu.CompilerParams(vmem_limit_bytes=VMEM_LIMIT),
        cost_estimate=pl.CostEstimate(flops=10 * 10 ** 9, bytes_accessed=8 * 10 ** 6, transcendentals=6 * 10 ** 6),
        name="attn_fwd",
    )(qkv, *tables)


def attn_bwd(qkv, dctx, lse, tables, first, count, done=None):
    n_seq, seq, _ = qkv.shape

    def rows(n, width):
        return pl.BlockSpec((None, n, width), lambda b: (b + first, 0, 0))

    ins = [qkv, dctx, lse, *tables]
    in_specs = [rows(seq, 512), rows(seq, 256), rows(8, seq)] + [table_spec(seq)] * 3
    kernel, aliases = attn_bwd_kernel, {}
    if done is not None:
        aliases = {len(ins): 0, len(ins) + 1: 1}
        ins += done
        in_specs += [pl.BlockSpec(memory_space=pl.ANY)] * 2

        def kernel(*refs):
            attn_bwd_kernel(*refs[:6], *refs[8:])

    return pl.pallas_call(
        kernel,
        grid=(count,),
        in_specs=in_specs,
        out_specs=[rows(seq, 512), rows(8, 512)],
        out_shape=[jax.ShapeDtypeStruct((n_seq, seq, 512), jnp.bfloat16),
                   jax.ShapeDtypeStruct((n_seq, 8, 512), jnp.float32)],
        scratch_shapes=[pltpu.VMEM((6, seq, LANES), jnp.float32)],
        input_output_aliases=aliases,
        compiler_params=pltpu.CompilerParams(vmem_limit_bytes=VMEM_LIMIT),
        cost_estimate=pl.CostEstimate(flops=15 * 10 ** 9, bytes_accessed=12 * 10 ** 6, transcendentals=6 * 10 ** 6),
        name="attn_bwd",
    )(*ins)


def rope_tables(rope_angle):
    cos_a, sin_a = jnp.cos(rope_angle), jnp.sin(rope_angle)
    rows = rope_angle.shape[0]
    zero = jnp.zeros((rows, HALF), jnp.float32)
    ones = jnp.ones((rows, LANES - 2 * HALF), jnp.float32)
    return (jnp.concatenate([cos_a, cos_a, ones], axis=1),
            jnp.concatenate([zero, sin_a, 0.0 * ones], axis=1),
            jnp.concatenate([-sin_a, zero, 0.0 * ones], axis=1))


def ring_perm(step):
    return [(RING[r] * 2 + c, RING[(r + step) % N_CHIP] * 2 + c) for r in range(N_CHIP) for c in range(2)]


PARTNER = [(t, t ^ 1) for t in range(2 * N_CHIP)]


def ring_place():
    tp = lax.axis_index('tp')
    chip, core = tp // 2, tp % 2
    return jnp.where(chip % 2 == 0, chip // 2, 7 - chip // 2), core


def chip_at(place):
    place = place % N_CHIP
    return jnp.where(place < 4, place * 2, 15 - place * 2)


def tie(values, after):
    return lax.optimization_barrier((*values, after))[:-1]


def exchange(part):
    n_seq, seq_len, depth = part.shape
    blk = seq_len // (2 * N_CHIP)
    _, core = ring_place()
    blocks = part.reshape(n_seq, N_CHIP, 2, blk, depth)
    theirs = lax.dynamic_slice_in_dim(blocks, 1 - core, 1, axis=2).reshape(n_seq, N_CHIP * blk, depth)
    return lax.ppermute(theirs, 'tp', PARTNER)


def both_weights(w_mat):
    return jnp.concatenate([w_mat, lax.ppermute(w_mat, 'tp', PARTNER)], axis=0)


def product_kernel(n_parts, idx_ref, *refs):
    del idx_ref
    w_ref, outs, rows_scr = refs[8 * n_parts], refs[8 * n_parts + 1:-1], refs[-1]
    blk = refs[0].shape[0]

    @pl.when(pl.program_id(0) == 0)
    def _():
        base = 0
        for p in range(n_parts):
            depth = refs[8 * p].shape[-1]
            for j in range(8):
                rows_scr[j * blk:(j + 1) * blk, base:base + depth] = refs[8 * p + j][...]
            base += depth

    acc = dot_nn(rows_scr[...], w_ref[...]).astype(jnp.bfloat16)
    for j in range(4):
        outs[j][...] = acc[2 * j * blk:2 * (j + 1) * blk].reshape(outs[j].shape)


def block_products(parts, others, w_mat, idx):
    n_seq, seq_len, _ = parts[0].shape
    depth, n_out = w_mat.shape
    blk, tile, half = seq_len // (2 * N_CHIP), 512, n_seq // 2
    in_specs, ins = [], []
    for kind, group in enumerate((parts, others)):
        for part in group:
            for hop in range(2):
                for seq in range(n_seq):
                    pos = hop * 4 + kind * 2 + seq // half
                    in_specs.append(pl.BlockSpec((None, blk, part.shape[-1]),
                                                 lambda n, idx, seq=seq, pos=pos: (seq, idx[pos], 0)))
                    ins.append(part)
    in_specs.append(pl.BlockSpec((depth, tile), lambda n, idx: (0, n)))
    out_spec = pl.BlockSpec((half, blk, tile), lambda n, idx: (0, 0, n))
    shape = jax.ShapeDtypeStruct((half, blk, n_out), jnp.bfloat16)
    n_parts = len(parts) + len(others)

    def kernel(*refs):
        product_kernel(n_parts, *refs)

    return pl.pallas_call(
        kernel,
        grid_spec=pltpu.PrefetchScalarGridSpec(
            num_scalar_prefetch=1, grid=(n_out // tile,), in_specs=in_specs, out_specs=[out_spec] * 4,
            scratch_shapes=[pltpu.VMEM((2 * n_seq * blk, depth), jnp.bfloat16)]),
        out_shape=[shape] * 4,
        compiler_params=pltpu.CompilerParams(vmem_limit_bytes=VMEM_LIMIT),
        cost_estimate=pl.CostEstimate(flops=4 * n_seq * blk * depth * n_out, bytes_accessed=2 * depth * n_out, transcendentals=0),
        name="block_products",
    )(idx, *ins, w_mat)


class RingSum:
    def __init__(self, parts, others, w_mat):
        self.operands = parts, others, w_mat
        self.place, self.core = ring_place()
        self.terms, self.got, self.step, self.token = {}, (), 0, None

    def product(self, first, after=None):
        idx = []
        for s in (first, first + 1):
            chips = [chip_at(self.place + side * (1 + s)) for side in (-1, 1)]
            idx += [2 * c + self.core for c in chips] + chips
        idx = jnp.stack(idx).astype(jnp.int32)
        if after is not None:
            idx, = tie((idx,), after)
        made = block_products(*self.operands, idx)
        self.terms[first], self.terms[first + 1] = made[:2], made[2:]

    def sums(self):
        terms = self.terms[self.step]
        if self.got:
            terms = [t.astype(jnp.float32) + g.astype(jnp.float32) for t, g in zip(terms, self.got)]
        return terms

    def send(self, after=()):
        sent = [t.astype(jnp.bfloat16) for t in self.sums()]
        for value in after:
            sent = tie(sent, value)
        sent = lax.optimization_barrier(tuple(sent))
        self.got = [lax.ppermute(t, 'tp', ring_perm(way)) for t, way in zip(sent, (1, -1))]
        self.token = sent[0]
        self.step += 1

    def close(self, made):
        self.got[0], self.got[1], *values = lax.optimization_barrier((*self.got, *made.values()))
        return dict(zip(made, values))

    def result(self):
        return jnp.concatenate(self.sums(), axis=0)


def small_all_reduce(t):
    for bit in (1, 2, 4, 8):
        t = t + lax.ppermute(t, 'tp', [(d, d ^ bit) for d in range(2 * N_CHIP)])
    return t


def rows_major(t):
    return with_layout_constraint(t, Layout(major_to_minor=tuple(range(t.ndim))))


def gather(t):
    return lax.all_gather(t, 'tp', axis=1, tiled=True)


def rows_dot(a, b):
    return jnp.einsum('bsd,de->bse', a, b, preferred_element_type=jnp.float32)


def rows_dot_t(a, b):
    return jnp.einsum('bse,fe->bsf', a, b, preferred_element_type=jnp.float32)


def outer_sum(a, b):
    return jnp.einsum('bsc,bse->ce', a, b, preferred_element_type=jnp.float32)


def layer_body(x_blk, rope_angle, ln_gain, ln_bias, w_q, b_q, w_k, b_k, w_v, b_v, w_o, b_o, w_up, b_up, w_down, b_down, dy_blk):
    normed, inv_std = norm_stats(x_blk)
    h_loc = (normed * ln_gain + ln_bias).astype(jnp.bfloat16)
    h_full, dy_full = gather(h_loc), gather(dy_blk)
    model_dim = x_blk.shape[-1]
    heads_loc, head_dim = b_q.shape
    width = heads_loc * head_dim
    tables = rope_tables(rope_angle)

    w_qkv = jnp.concatenate([w_q, w_k, w_v, jnp.zeros((model_dim, 32), jnp.bfloat16)], axis=1)
    b_qkv = jnp.concatenate([b_q.reshape(-1), b_k.reshape(-1), b_v.reshape(-1), jnp.zeros((32,), jnp.float32)])
    w_o_pad = jnp.concatenate([w_o, jnp.zeros((256 - width, model_dim), jnp.bfloat16)], axis=0)
    w_out = rows_major(jnp.concatenate([w_o_pad, w_down], axis=0))
    w_in_t = rows_major(jnp.concatenate([w_qkv, w_up], axis=1).T)
    w_out, w_in_t = both_weights(w_out), both_weights(w_in_t)
    h_full, w_qkv, w_out, w_in_t, b_qkv, *tables = lax.optimization_barrier(
        (h_full, w_qkv, w_out, w_in_t, b_qkv, *tables))

    qkv = (rows_dot(h_full, w_qkv) + b_qkv).astype(jnp.bfloat16)
    ctx, lse = attn_fwd(qkv, tables)
    act_f, gelu_pull = jax.vjp(gelu_tanh, rows_dot(h_full, w_up) + b_up)
    act = rows_major(act_f.astype(jnp.bfloat16))
    out = {}

    def run_dctx(token):
        dy_t, = tie((dy_full,), token)
        return {'d_ctx': rows_dot_t(dy_t, w_o_pad).astype(jnp.bfloat16)}

    def run_attn_a(token):
        d_ctx, = tie((out['d_ctx'],), token)
        return dict(zip(('d_qkv', 'd_bias'), attn_bwd(qkv, d_ctx, lse, tables, 0, 2)))

    def run_attn_b(token):
        d_ctx, = tie((out['d_ctx'],), token)
        return dict(zip(('d_qkv', 'd_bias'), attn_bwd(qkv, d_ctx, lse, tables, 2, 2, [out['d_qkv'], out['d_bias']])))

    def run_act(token):
        dy_t, = tie((dy_full,), token)
        d_pre = gelu_pull(rows_dot_t(dy_t, w_down))[0]
        return {'grad_bup': jnp.sum(d_pre, axis=(0, 1)), 'd_pre': rows_major(d_pre.astype(jnp.bfloat16))}

    def run_wdown(token):
        act_t, = tie((act,), token)
        return {'wdown': outer_sum(act_t, dy_full)}

    def run_wo(token):
        ctx_t, = tie((ctx,), token)
        return {'wo': outer_sum(ctx_t, dy_full)[:width]}

    def run_wqkv(token):
        d_qkv, = tie((out['d_qkv'],), token)
        grad = outer_sum(d_qkv, h_full)
        return {name: grad[j * width:(j + 1) * width] for j, name in enumerate(('wq', 'wk', 'wv'))}

    def run_wup(token):
        d_pre, = tie((out['d_pre'],), token)
        return {'wup': outer_sum(h_full, d_pre)}

    ring_y = RingSum((ctx, act), (exchange(ctx), exchange(act)), w_out)
    for first in range(0, N_CHIP, 2):
        ring_y.product(first, ring_y.terms[first - 1][0] if first else None)
    after = (dy_full, ring_y.terms[N_CHIP - 1][0])
    for run in (run_dctx, run_attn_a, run_attn_b, run_act):
        ring_y.send(after)
        out.update(ring_y.close(run(ring_y.token)))
        after = ()

    ring_h = RingSum((out['d_qkv'], out['d_pre']), (exchange(out['d_qkv']), exchange(out['d_pre'])), w_in_t)
    ring_y.send()
    ring_h.product(0, ring_y.token)
    ring_h.terms[0] = list(ring_y.close({j: t for j, t in enumerate(ring_h.terms[0])}).values())

    def both_hops(runs, first=None):
        ring_y.send()
        ring_h.send((ring_y.token,))
        made = {}
        if first is not None:
            ring_h.product(first, ring_h.token)
            made = {'term': ring_h.terms[first][0]}
        for run in runs:
            made.update(run(ring_h.token))
        made = ring_y.close(ring_h.close(made))
        if first is not None:
            ring_h.terms[first] = [made.pop('term'), ring_h.terms[first][1]]
        out.update(made)

    both_hops((run_wo,), 2)
    both_hops((run_wdown,))
    for first, run in ((4, None), (None, run_wqkv), (6, None), (None, run_wup), (None, None)):
        ring_h.send()
        if first is not None:
            ring_h.product(first, ring_h.token)
        if run is not None:
            out.update(ring_h.close(run(ring_h.token)))
    branch_sum, d_h_loc = ring_y.result(), ring_h.result()
    y_blk = (x_blk.astype(jnp.float32) + branch_sum + b_o + b_down).astype(jnp.bfloat16)
    dy_f = dy_blk.astype(jnp.float32)
    grad_wq, grad_wk, grad_wv = out['wq'].T, out['wk'].T, out['wv'].T
    grad_wo, grad_wup, grad_wdown, grad_bup = out['wo'], out['wup'], out['wdown'], out['grad_bup']
    grad_b = jnp.sum(out['d_bias'][:, 0, :], axis=0)
    grad_bq, grad_bk, grad_bv = (grad_b[j * width:(j + 1) * width].reshape(heads_loc, head_dim) for j in range(3))

    small_sums = small_all_reduce(jnp.stack([jnp.sum(d_h_loc * normed, axis=(0, 1)), jnp.sum(d_h_loc, axis=(0, 1)),
                                             jnp.sum(dy_f, axis=(0, 1))]))
    d_x = dy_f + norm_backward(d_h_loc, normed, inv_std, ln_gain)
    return (y_blk, d_x, small_sums[0], small_sums[1], grad_wq, grad_bq, grad_wk, grad_bk,
            grad_wv, grad_bv, grad_wo, small_sums[2], grad_wup, grad_bup, grad_wdown, small_sums[2])


def solution(mesh):
    row_spec = P('dp', 'tp', None)
    col_spec = P(None, 'tp')
    head_spec = P('tp', None)
    grad_cols = P('dp', 'tp')
    grad_rows = P(('dp', 'tp'), None)
    in_specs = (row_spec, P(None, None), P(None), P(None), col_spec, head_spec, col_spec, head_spec,
                col_spec, head_spec, P('tp', None), P(None), col_spec, P('tp'), P('tp', None), P(None), row_spec)
    out_specs = (row_spec, row_spec, P('dp'), P('dp'), grad_cols, grad_rows, grad_cols, grad_rows, grad_cols,
                 grad_rows, grad_rows, P('dp'), grad_cols, P(('dp', 'tp')), grad_rows, P('dp'))
    return jax.shard_map(layer_body, mesh=mesh, in_specs=in_specs, out_specs=out_specs, check_vma=False)
```

```python
import jax
import jax.numpy as jnp
from jax import lax
from jax.experimental import pallas as pl
from jax.experimental.layout import Layout, with_layout_constraint
from jax.experimental.pallas import tpu as pltpu
from jax.sharding import PartitionSpec as P

LN_EPS = 1e-5
HEAD = 80
HALF = 32
LANES = 128
Q_BLK = 256
RING = (0, 2, 4, 6, 7, 5, 3, 1)
N_CHIP = 8
VMEM_LIMIT = 60 * 2 ** 20


def norm_stats(x_blk):
    x_f = x_blk.astype(jnp.float32)
    centered = x_f - jnp.mean(x_f, axis=-1, keepdims=True)
    inv_std = lax.rsqrt(jnp.mean(centered * centered, axis=-1, keepdims=True) + LN_EPS)
    return centered * inv_std, inv_std


def norm_backward(d_h, normed, inv_std, ln_gain):
    d_norm = d_h * ln_gain
    return inv_std * (d_norm - jnp.mean(d_norm, axis=-1, keepdims=True)
                      - normed * jnp.mean(d_norm * normed, axis=-1, keepdims=True))


def gelu_tanh(t):
    return jax.nn.gelu(t, approximate=True)


def lane_iota(rows):
    return lax.broadcasted_iota(jnp.int32, (rows, LANES), 1)


def unpack_head(ref, offset):
    rows = ref.shape[0]
    col, shift = offset // LANES, offset % LANES
    lane = lane_iota(rows)
    head = ref[:, col * LANES:(col + 1) * LANES].astype(jnp.float32)
    if shift:
        head = pltpu.roll(head, LANES - shift, 1)
        if shift + HEAD > LANES:
            after = pltpu.roll(ref[:, (col + 1) * LANES:(col + 2) * LANES].astype(jnp.float32), LANES - shift, 1)
            head = jnp.where(lane < LANES - shift, head, after)
    return jnp.where(lane < HEAD, head, 0.0)


def pack_heads(heads, n_cols):
    rows = heads[0].shape[0]
    lane = lane_iota(rows)
    cols = [None] * n_cols
    for idx, head in enumerate(heads):
        offset = idx * HEAD
        col, shift = offset // LANES, offset % LANES
        moved = pltpu.roll(head, shift, 1) if shift else head
        low = (lane >= shift) & (lane < shift + HEAD)
        cols[col] = jnp.where(low, moved, 0.0 if cols[col] is None else cols[col])
        if shift + HEAD > LANES:
            cols[col + 1] = jnp.where(lane < shift + HEAD - LANES, moved, 0.0)
    return cols


def rotate(t, cos_t, sin_up, sin_down):
    return t * cos_t + pltpu.roll(t, HALF, 1) * sin_up + pltpu.roll(t, LANES - HALF, 1) * sin_down


def dot_nt(a, b):
    return lax.dot_general(a, b, (((1,), (1,)), ((), ())), preferred_element_type=jnp.float32)


def dot_nn(a, b):
    return jnp.dot(a, b, preferred_element_type=jnp.float32)


def causal(hi, lo):
    key = lax.broadcasted_iota(jnp.int32, (hi, Q_BLK), 0)
    query = lax.broadcasted_iota(jnp.int32, (hi, Q_BLK), 1) + lo
    return key <= query


def attn_fwd_kernel(qkv_ref, cos_ref, up_ref, down_ref, ctx_ref, lse_ref, head_scr):
    seq = qkv_ref.shape[0]
    scale = HEAD ** -0.5
    cos_t, sin_up, sin_down = cos_ref[...], up_ref[...], down_ref[...]
    lse_ref[...] = jnp.zeros_like(lse_ref)
    for h in range(2):
        q = rotate(unpack_head(qkv_ref, h * HEAD), cos_t, sin_up, sin_down).astype(jnp.bfloat16)
        k = rotate(unpack_head(qkv_ref, (2 + h) * HEAD), cos_t, sin_up, sin_down).astype(jnp.bfloat16)
        v_t = unpack_head(qkv_ref, (4 + h) * HEAD).T.astype(jnp.bfloat16)
        for lo in range(0, seq, Q_BLK):
            hi = lo + Q_BLK
            s_t = dot_nt(k[:hi], q[lo:hi]) * scale
            s_t = jnp.where(causal(hi, lo), s_t, -1e30)
            top = jnp.max(s_t, axis=0, keepdims=True)
            e_t = jnp.exp(s_t - top)
            total = jnp.sum(e_t, axis=0, keepdims=True)
            p_t = (e_t * (1.0 / total)).astype(jnp.bfloat16)
            head_scr[h, lo:hi, :] = dot_nn(v_t[:, :hi], p_t).T
            lse_ref[h:h + 1, lo:hi] = top + jnp.log(total)
    cols = pack_heads([head_scr[0], head_scr[1]], 2)
    for c in range(2):
        ctx_ref[:, c * LANES:(c + 1) * LANES] = cols[c].astype(jnp.bfloat16)


def attn_bwd_kernel(qkv_ref, dctx_ref, lse_ref, cos_ref, up_ref, down_ref, dqkv_ref, dbias_ref, d_scr):
    seq = qkv_ref.shape[0]
    scale = HEAD ** -0.5
    cos_t, sin_up, sin_down = cos_ref[...], up_ref[...], down_ref[...]
    for h in range(2):
        q = rotate(unpack_head(qkv_ref, h * HEAD), cos_t, sin_up, sin_down).astype(jnp.bfloat16)
        k_f = rotate(unpack_head(qkv_ref, (2 + h) * HEAD), cos_t, sin_up, sin_down)
        k = k_f.astype(jnp.bfloat16)
        k_t = k_f.T.astype(jnp.bfloat16)
        v = unpack_head(qkv_ref, (4 + h) * HEAD).astype(jnp.bfloat16)
        dctx = unpack_head(dctx_ref, h * HEAD).astype(jnp.bfloat16)
        for lo in reversed(range(0, seq, Q_BLK)):
            hi = lo + Q_BLK
            s_t = dot_nt(k[:hi], q[lo:hi]) * scale
            p_t = jnp.where(causal(hi, lo), jnp.exp(s_t - lse_ref[h:h + 1, lo:hi]), 0.0)
            dp_t = dot_nt(v[:hi], dctx[lo:hi])
            row = jnp.sum(dp_t * p_t, axis=0, keepdims=True)
            ds_t = (p_t * (dp_t - row) * scale).astype(jnp.bfloat16)
            d_scr[h, lo:hi, :] = dot_nn(k_t[:, :hi], ds_t).T
            dk_part = dot_nn(ds_t, q[lo:hi])
            dv_part = dot_nn(p_t.astype(jnp.bfloat16), dctx[lo:hi])
            if hi == seq:
                d_scr[2 + h] = dk_part
                d_scr[4 + h] = dv_part
            else:
                d_scr[2 + h, :hi, :] += dk_part
                d_scr[4 + h, :hi, :] += dv_part
    heads = [rotate(d_scr[j], cos_t, -sin_up, -sin_down) for j in range(4)] + [d_scr[4], d_scr[5]]
    cols = pack_heads(heads, 4)
    for c in range(4):
        span = slice(c * LANES, (c + 1) * LANES)
        dqkv_ref[:, span] = cols[c].astype(jnp.bfloat16)
        dbias_ref[:, span] = jnp.broadcast_to(jnp.sum(cols[c], axis=0, keepdims=True), (8, LANES))


def seq_spec(rows, width):
    return pl.BlockSpec((None, rows, width), lambda b: (b, 0, 0))


def table_spec(rows):
    return pl.BlockSpec((rows, LANES), lambda b: (0, 0))


def attn_fwd(qkv, tables):
    n_seq, seq, _ = qkv.shape
    return pl.pallas_call(
        attn_fwd_kernel,
        grid=(n_seq,),
        in_specs=[seq_spec(seq, 512)] + [table_spec(seq)] * 3,
        out_specs=[seq_spec(seq, 256), seq_spec(8, seq)],
        out_shape=[jax.ShapeDtypeStruct((n_seq, seq, 256), jnp.bfloat16),
                   jax.ShapeDtypeStruct((n_seq, 8, seq), jnp.float32)],
        scratch_shapes=[pltpu.VMEM((2, seq, LANES), jnp.float32)],
        compiler_params=pltpu.CompilerParams(vmem_limit_bytes=VMEM_LIMIT),
        cost_estimate=pl.CostEstimate(flops=10 * 10 ** 9, bytes_accessed=8 * 10 ** 6, transcendentals=6 * 10 ** 6),
        name="attn_fwd",
    )(qkv, *tables)


def attn_bwd(qkv, dctx, lse, tables, first, count, done=None):
    n_seq, seq, _ = qkv.shape

    def rows(n, width):
        return pl.BlockSpec((None, n, width), lambda b: (b + first, 0, 0))

    ins = [qkv, dctx, lse, *tables]
    in_specs = [rows(seq, 512), rows(seq, 256), rows(8, seq)] + [table_spec(seq)] * 3
    kernel, aliases = attn_bwd_kernel, {}
    if done is not None:
        aliases = {len(ins): 0, len(ins) + 1: 1}
        ins += done
        in_specs += [pl.BlockSpec(memory_space=pl.ANY)] * 2

        def kernel(*refs):
            attn_bwd_kernel(*refs[:6], *refs[8:])

    return pl.pallas_call(
        kernel,
        grid=(count,),
        in_specs=in_specs,
        out_specs=[rows(seq, 512), rows(8, 512)],
        out_shape=[jax.ShapeDtypeStruct((n_seq, seq, 512), jnp.bfloat16),
                   jax.ShapeDtypeStruct((n_seq, 8, 512), jnp.float32)],
        scratch_shapes=[pltpu.VMEM((6, seq, LANES), jnp.float32)],
        input_output_aliases=aliases,
        compiler_params=pltpu.CompilerParams(vmem_limit_bytes=VMEM_LIMIT),
        cost_estimate=pl.CostEstimate(flops=15 * 10 ** 9, bytes_accessed=12 * 10 ** 6, transcendentals=6 * 10 ** 6),
        name="attn_bwd",
    )(*ins)


def rope_tables(rope_angle):
    cos_a, sin_a = jnp.cos(rope_angle), jnp.sin(rope_angle)
    rows = rope_angle.shape[0]
    zero = jnp.zeros((rows, HALF), jnp.float32)
    ones = jnp.ones((rows, LANES - 2 * HALF), jnp.float32)
    return (jnp.concatenate([cos_a, cos_a, ones], axis=1),
            jnp.concatenate([zero, sin_a, 0.0 * ones], axis=1),
            jnp.concatenate([-sin_a, zero, 0.0 * ones], axis=1))


def ring_perm(step):
    return [(RING[r] * 2 + c, RING[(r + step) % N_CHIP] * 2 + c) for r in range(N_CHIP) for c in range(2)]


PARTNER = [(t, t ^ 1) for t in range(2 * N_CHIP)]


def ring_place():
    tp = lax.axis_index('tp')
    chip, core = tp // 2, tp % 2
    return jnp.where(chip % 2 == 0, chip // 2, 7 - chip // 2), core


def chip_at(place):
    place = place % N_CHIP
    return jnp.where(place < 4, place * 2, 15 - place * 2)


def tie(values, after):
    return lax.optimization_barrier((*values, after))[:-1]


def exchange(part):
    n_seq, seq_len, depth = part.shape
    blk = seq_len // (2 * N_CHIP)
    _, core = ring_place()
    blocks = part.reshape(n_seq, N_CHIP, 2, blk, depth)
    theirs = lax.dynamic_slice_in_dim(blocks, 1 - core, 1, axis=2).reshape(n_seq, N_CHIP * blk, depth)
    return lax.ppermute(theirs, 'tp', PARTNER)


def both_weights(w_mat):
    return jnp.concatenate([w_mat, lax.ppermute(w_mat, 'tp', PARTNER)], axis=0)


def product_kernel(n_parts, idx_ref, *refs):
    del idx_ref
    w_ref, outs, rows_scr = refs[8 * n_parts], refs[8 * n_parts + 1:-1], refs[-1]
    blk = refs[0].shape[0]

    @pl.when(pl.program_id(0) == 0)
    def _():
        base = 0
        for p in range(n_parts):
            depth = refs[8 * p].shape[-1]
            for j in range(8):
                rows_scr[j * blk:(j + 1) * blk, base:base + depth] = refs[8 * p + j][...]
            base += depth

    acc = dot_nn(rows_scr[...], w_ref[...]).astype(jnp.bfloat16)
    for j in range(4):
        outs[j][...] = acc[2 * j * blk:2 * (j + 1) * blk].reshape(outs[j].shape)


def block_products(parts, others, w_mat, idx):
    n_seq, seq_len, _ = parts[0].shape
    depth, n_out = w_mat.shape
    blk, tile, half = seq_len // (2 * N_CHIP), 512, n_seq // 2
    in_specs, ins = [], []
    for kind, group in enumerate((parts, others)):
        for part in group:
            for hop in range(2):
                for seq in range(n_seq):
                    pos = hop * 4 + kind * 2 + seq // half
                    in_specs.append(pl.BlockSpec((None, blk, part.shape[-1]),
                                                 lambda n, idx, seq=seq, pos=pos: (seq, idx[pos], 0)))
                    ins.append(part)
    in_specs.append(pl.BlockSpec((depth, tile), lambda n, idx: (0, n)))
    out_spec = pl.BlockSpec((half, blk, tile), lambda n, idx: (0, 0, n))
    shape = jax.ShapeDtypeStruct((half, blk, n_out), jnp.bfloat16)
    n_parts = len(parts) + len(others)

    def kernel(*refs):
        product_kernel(n_parts, *refs)

    return pl.pallas_call(
        kernel,
        grid_spec=pltpu.PrefetchScalarGridSpec(
            num_scalar_prefetch=1, grid=(n_out // tile,), in_specs=in_specs, out_specs=[out_spec] * 4,
            scratch_shapes=[pltpu.VMEM((2 * n_seq * blk, depth), jnp.bfloat16)]),
        out_shape=[shape] * 4,
        compiler_params=pltpu.CompilerParams(vmem_limit_bytes=VMEM_LIMIT),
        cost_estimate=pl.CostEstimate(flops=4 * n_seq * blk * depth * n_out, bytes_accessed=2 * depth * n_out, transcendentals=0),
        name="block_products",
    )(idx, *ins, w_mat)


class RingSum:
    def __init__(self, parts, others, w_mat):
        self.operands = parts, others, w_mat
        self.place, self.core = ring_place()
        self.terms, self.got, self.step, self.token = {}, (), 0, None

    def product(self, first, after=None):
        idx = []
        for s in (first, first + 1):
            chips = [chip_at(self.place + side * (1 + s)) for side in (-1, 1)]
            idx += [2 * c + self.core for c in chips] + chips
        idx = jnp.stack(idx).astype(jnp.int32)
        if after is not None:
            idx, = tie((idx,), after)
        made = block_products(*self.operands, idx)
        self.terms[first], self.terms[first + 1] = made[:2], made[2:]

    def sums(self):
        terms = self.terms[self.step]
        if self.got:
            terms = [t.astype(jnp.float32) + g.astype(jnp.float32) for t, g in zip(terms, self.got)]
        return terms

    def send(self, after=()):
        sent = [t.astype(jnp.bfloat16) for t in self.sums()]
        for value in after:
            sent = tie(sent, value)
        sent = lax.optimization_barrier(tuple(sent))
        self.got = [lax.ppermute(t, 'tp', ring_perm(way)) for t, way in zip(sent, (1, -1))]
        self.token = sent[0]
        self.step += 1

    def close(self, made):
        self.got[0], self.got[1], *values = lax.optimization_barrier((*self.got, *made.values()))
        return dict(zip(made, values))

    def result(self):
        return jnp.concatenate(self.sums(), axis=0)


def small_all_reduce(t):
    for bit in (1, 2, 4, 8):
        t = t + lax.ppermute(t, 'tp', [(d, d ^ bit) for d in range(2 * N_CHIP)])
    return t


def rows_major(t):
    return with_layout_constraint(t, Layout(major_to_minor=tuple(range(t.ndim))))


def gather(t):
    return lax.all_gather(t, 'tp', axis=1, tiled=True)


def rows_dot(a, b):
    return jnp.einsum('bsd,de->bse', a, b, preferred_element_type=jnp.float32)


def rows_dot_t(a, b):
    return jnp.einsum('bse,fe->bsf', a, b, preferred_element_type=jnp.float32)


def outer_sum(a, b):
    return jnp.einsum('bsc,bse->ce', a, b, preferred_element_type=jnp.float32)


def layer_body(x_blk, rope_angle, ln_gain, ln_bias, w_q, b_q, w_k, b_k, w_v, b_v, w_o, b_o, w_up, b_up, w_down, b_down, dy_blk):
    normed, inv_std = norm_stats(x_blk)
    h_loc = (normed * ln_gain + ln_bias).astype(jnp.bfloat16)
    h_full, dy_full = gather(h_loc), gather(dy_blk)
    model_dim = x_blk.shape[-1]
    heads_loc, head_dim = b_q.shape
    width = heads_loc * head_dim
    tables = rope_tables(rope_angle)

    w_qkv = jnp.concatenate([w_q, w_k, w_v, jnp.zeros((model_dim, 32), jnp.bfloat16)], axis=1)
    b_qkv = jnp.concatenate([b_q.reshape(-1), b_k.reshape(-1), b_v.reshape(-1), jnp.zeros((32,), jnp.float32)])
    w_o_pad = jnp.concatenate([w_o, jnp.zeros((256 - width, model_dim), jnp.bfloat16)], axis=0)
    w_out = rows_major(jnp.concatenate([w_o_pad, w_down], axis=0))
    w_in_t = rows_major(jnp.concatenate([w_qkv, w_up], axis=1).T)
    w_out, w_in_t = both_weights(w_out), both_weights(w_in_t)
    h_full, w_qkv, w_out, w_in_t, b_qkv, *tables = lax.optimization_barrier(
        (h_full, w_qkv, w_out, w_in_t, b_qkv, *tables))

    qkv = (rows_dot(h_full, w_qkv) + b_qkv).astype(jnp.bfloat16)
    ctx, lse = attn_fwd(qkv, tables)
    act_f, gelu_pull = jax.vjp(gelu_tanh, rows_dot(h_full, w_up) + b_up)
    act = rows_major(act_f.astype(jnp.bfloat16))
    out = {}

    def run_dctx(token):
        dy_t, = tie((dy_full,), token)
        return {'d_ctx': rows_dot_t(dy_t, w_o_pad).astype(jnp.bfloat16)}

    def run_attn_a(token):
        d_ctx, = tie((out['d_ctx'],), token)
        return dict(zip(('d_qkv', 'd_bias'), attn_bwd(qkv, d_ctx, lse, tables, 0, 2)))

    def run_attn_b(token):
        d_ctx, = tie((out['d_ctx'],), token)
        return dict(zip(('d_qkv', 'd_bias'), attn_bwd(qkv, d_ctx, lse, tables, 2, 2, [out['d_qkv'], out['d_bias']])))

    def run_act(token):
        dy_t, = tie((dy_full,), token)
        d_pre = gelu_pull(rows_dot_t(dy_t, w_down))[0]
        return {'grad_bup': jnp.sum(d_pre, axis=(0, 1)), 'd_pre': rows_major(d_pre.astype(jnp.bfloat16))}

    def run_wdown(token):
        act_t, = tie((act,), token)
        return {'wdown': outer_sum(act_t, dy_full)}

    def run_wo(token):
        ctx_t, = tie((ctx,), token)
        return {'wo': outer_sum(ctx_t, dy_full)[:width]}

    def run_wqkv(token):
        d_qkv, = tie((out['d_qkv'],), token)
        grad = outer_sum(d_qkv, h_full)
        return {name: grad[j * width:(j + 1) * width] for j, name in enumerate(('wq', 'wk', 'wv'))}

    def run_wup(token):
        d_pre, = tie((out['d_pre'],), token)
        return {'wup': outer_sum(h_full, d_pre)}

    ring_y = RingSum((ctx, act), (exchange(ctx), exchange(act)), w_out)
    for first in range(0, N_CHIP, 2):
        ring_y.product(first, ring_y.terms[first - 1][0] if first else None)
    after = (dy_full, ring_y.terms[N_CHIP - 3][0])
    for run in (run_dctx, run_attn_a, run_attn_b, run_act):
        ring_y.send(after)
        out.update(ring_y.close(run(ring_y.token)))
        after = ()

    ring_h = RingSum((out['d_qkv'], out['d_pre']), (exchange(out['d_qkv']), exchange(out['d_pre'])), w_in_t)
    ring_y.send()
    ring_h.product(0, ring_y.token)
    ring_h.terms[0] = list(ring_y.close({j: t for j, t in enumerate(ring_h.terms[0])}).values())

    def both_hops(runs, first=None):
        ring_y.send()
        ring_h.send((ring_y.token,))
        made = {}
        if first is not None:
            ring_h.product(first, ring_h.token)
            made = {'term': ring_h.terms[first][0]}
        for run in runs:
            made.update(run(ring_h.token))
        made = ring_y.close(ring_h.close(made))
        if first is not None:
            ring_h.terms[first] = [made.pop('term'), ring_h.terms[first][1]]
        out.update(made)

    both_hops((run_wo,), 2)
    both_hops((run_wdown,))
    for first, run in ((4, None), (None, run_wqkv), (6, None), (None, run_wup), (None, None)):
        ring_h.send()
        if first is not None:
            ring_h.product(first, ring_h.token)
        if run is not None:
            out.update(ring_h.close(run(ring_h.token)))
    branch_sum, d_h_loc = ring_y.result(), ring_h.result()
    y_blk = (x_blk.astype(jnp.float32) + branch_sum + b_o + b_down).astype(jnp.bfloat16)
    dy_f = dy_blk.astype(jnp.float32)
    grad_wq, grad_wk, grad_wv = out['wq'].T, out['wk'].T, out['wv'].T
    grad_wo, grad_wup, grad_wdown, grad_bup = out['wo'], out['wup'], out['wdown'], out['grad_bup']
    grad_b = jnp.sum(out['d_bias'][:, 0, :], axis=0)
    grad_bq, grad_bk, grad_bv = (grad_b[j * width:(j + 1) * width].reshape(heads_loc, head_dim) for j in range(3))

    small_sums = small_all_reduce(jnp.stack([jnp.sum(d_h_loc * normed, axis=(0, 1)), jnp.sum(d_h_loc, axis=(0, 1)),
                                             jnp.sum(dy_f, axis=(0, 1))]))
    d_x = dy_f + norm_backward(d_h_loc, normed, inv_std, ln_gain)
    return (y_blk, d_x, small_sums[0], small_sums[1], grad_wq, grad_bq, grad_wk, grad_bk,
            grad_wv, grad_bv, grad_wo, small_sums[2], grad_wup, grad_bup, grad_wdown, small_sums[2])


def solution(mesh):
    row_spec = P('dp', 'tp', None)
    col_spec = P(None, 'tp')
    head_spec = P('tp', None)
    grad_cols = P('dp', 'tp')
    grad_rows = P(('dp', 'tp'), None)
    in_specs = (row_spec, P(None, None), P(None), P(None), col_spec, head_spec, col_spec, head_spec,
                col_spec, head_spec, P('tp', None), P(None), col_spec, P('tp'), P('tp', None), P(None), row_spec)
    out_specs = (row_spec, row_spec, P('dp'), P('dp'), grad_cols, grad_rows, grad_cols, grad_rows, grad_cols,
                 grad_rows, grad_rows, P('dp'), grad_cols, P(('dp', 'tp')), grad_rows, P('dp'))
    return jax.shard_map(layer_body, mesh=mesh, in_specs=in_specs, out_specs=out_specs, check_vma=False)
```
